32 devices in a mesh: groups: 2 (over x), traces: 16 (over z, y, core).
Axes of the slice: x: 2, y: 2, z: 4, core: 2. Of those that a mesh axis runs over, the one named last changes fastest.
Arguments:
- raw_traces: float32 [8192, 8192], P(('groups', 'traces')), parts along dimension 0, may hold values from -6 to 6
- filter_index: int32 [8192], P(('groups', 'traces')), parts along dimension 0, may hold values from 0 to 255
- channel_order: int32 [512], P('groups'), parts along dimension 0, may hold values from 0 to 255, each once
- wavelets: float32 [256, 256], P('traces'), may hold values from -0.375 to 0.375
- damping: float32 [256], P('traces'), may hold values from 0.02 to 0.5
Outputs:
- deconvolved: float32 [8192, 8192], P(('groups', 'traces')), parts along dimension 0
The draws below stay inside these ranges and needn't reach their ends.
There are 2 independent parts, one for each index of `groups`. The reference program is written for one: setup_inputs(seed, part) draws one part's arguments, and reference() takes and returns one part's arrays. A program takes and returns all parts, laid end to end along the dimension named above; an argument that names none is the same for every part. Nothing has to cross between parts.
Inputs may be any that keep to these rules, and one draw needn't show every extreme that they name: `channel_order`: each of 0 to 255 appears once.
All inputs are finite; a program needn't handle non-finite values.
Results may differ from the reference program's by a relative error of at most 0.00021.
Values sent between devices are 32-bit elements; how exact they have to be, the bound alone decides.
A program may use at most 192 MiB of HBM per device.

```python
import math
import jax
import jax.numpy as jnp
from jax import lax

L = 8192
FILTERS = 256
FLEN = 256
TR_DEV = 256
TRACES = 4096
N_TRACES = 16


def plant(drawn, own_key, smallest, largest):
    longest = drawn.shape.index(max(drawn.shape))
    spots = []
    for shift in (0, 1):
        where = [jax.random.randint(jax.random.fold_in(own_key, axis), (), 0, length) for axis, length in enumerate(drawn.shape)]
        where[longest] = (where[longest] + shift) % drawn.shape[longest]
        spots.append(tuple(where))
    return drawn.at[spots[0]].set(smallest).at[spots[1]].set(largest)


def block_scale(key, shape, pieces, least, largest):
    factor_of, own = 1.0, jax.random.fold_in(key, 6)
    for dim, blocks in pieces:
        steps = jnp.exp(jax.random.uniform(jax.random.fold_in(own, dim), (blocks,), jnp.float32, least / len(pieces), largest / len(pieces)))
        factor_of = factor_of * jnp.repeat(steps, shape[dim] // blocks).reshape([-1 if axis == dim else 1 for axis in range(len(shape))])
    return factor_of


def centred(key, dims, deviation, bound, pieces=(), kind=jnp.bfloat16):
    loudness = block_scale(key, dims, pieces, -0.22, 0.18) if pieces else 1.0
    array = jax.random.normal(key, dims, jnp.float32) * deviation * loudness
    return jnp.minimum(jnp.maximum(array, -bound), bound).astype(kind)


def setup_inputs(seed: int = 0, part: int = 0) -> dict:
    streams_of = jax.random.split(jax.random.key(seed), 6)
    part_keys = jax.random.split(jax.random.fold_in(streams_of[5], part), 6)
    return {
        "raw_traces": centred(part_keys[0], (TRACES, L), 1.0, 6.0, ((0, 16),), jnp.float32),
        "filter_index": plant(jax.random.randint(part_keys[1], (TRACES,), 0, FILTERS), jax.random.fold_in(part_keys[1], 1), 0, FILTERS - 1).astype(jnp.int32),
        "channel_order": jax.random.permutation(part_keys[2], TR_DEV).astype(jnp.int32),
        "wavelets": centred(streams_of[3], (FILTERS, FLEN), FLEN ** -0.5, 0.375, ((0, 16),), jnp.float32),
        "damping": jnp.clip(jnp.exp(math.log(0.5) - 3.218876 * jax.random.uniform(streams_of[4], (FILTERS,), jnp.float32) ** block_scale(streams_of[4], (FILTERS,), ((0, 16),), -0.2, 0.2)), 0.02, 0.5),
    }


def filter_gains(wavelets, damping):
    padded = jnp.pad(wavelets, ((0, 0), (0, L - FLEN)))
    spectrum = jnp.fft.fft(padded, axis=1)
    spec_re = jnp.real(spectrum)
    spec_im = jnp.imag(spectrum)
    power = spec_re * spec_re + spec_im * spec_im
    level = jnp.mean(power, axis=1, keepdims=True)
    denom = power + damping[:, None] * (level + 1e-6)
    return spec_re / denom, -spec_im / denom


def reference(raw_traces, filter_index, channel_order, wavelets, damping):
    gain_re, gain_im = filter_gains(wavelets, damping)
    blocks = raw_traces.reshape(N_TRACES, TR_DEV, L)
    picks = filter_index.reshape(N_TRACES, TR_DEV)

    def one_block(pair):
        rows, index = pair
        spectrum = jnp.fft.fft(rows, axis=1)
        spec_re = jnp.real(spectrum)
        spec_im = jnp.imag(spectrum)
        pick_re = jnp.take(gain_re, index, axis=0)
        pick_im = jnp.take(gain_im, index, axis=0)
        out_re = spec_re * pick_re - spec_im * pick_im
        out_im = spec_re * pick_im + spec_im * pick_re
        return jnp.real(jnp.fft.ifft(lax.complex(out_re, out_im), axis=1))

    results = lax.map(one_block, (blocks, picks)).reshape(TRACES, L)
    out_rows = jnp.arange(TRACES, dtype=jnp.int32)
    position = (out_rows // TR_DEV) * TR_DEV + jnp.take(channel_order, out_rows % TR_DEV).astype(jnp.int32)
    source = ((position % N_TRACES) * TR_DEV + position // N_TRACES).astype(jnp.int32)
    return jnp.take(results, source, axis=0)
```

```python
import functools
import math

import jax
import jax.numpy as jnp
import numpy as np
from jax import lax
from jax.experimental import pallas as pl
from jax.experimental.pallas import tpu as pltpu
from jax.sharding import PartitionSpec as P

LANES = 128
RADIX = 8
ROWS = 16

KEPT = (
    [RADIX * b for b in range(RADIX // 2 + 1)]
    + [a + RADIX * b for a in range(1, RADIX // 2) for b in range(RADIX)]
    + [RADIX // 2 + RADIX * b for b in range(RADIX // 2)]
)
SLOT = {k: s for s, k in enumerate(KEPT)}
KEEP = len(KEPT)


def split_np(table):
    high = jnp.asarray(table, jnp.float32).astype(jnp.bfloat16)
    low = (jnp.asarray(table, jnp.float32) - high.astype(jnp.float32)).astype(jnp.bfloat16)
    return high, low


def lane_matrix(sign, scale):
    ids = np.arange(LANES)
    angle = 2.0 * np.pi * (np.outer(ids, ids) % LANES) / LANES
    c, s = np.cos(angle) * scale, sign * np.sin(angle) * scale
    full = np.block([[c, s], [-s, c]])
    import ml_dtypes

    high = full.astype(np.float32).astype(ml_dtypes.bfloat16)
    low = (full.astype(np.float32) - high.astype(np.float32)).astype(ml_dtypes.bfloat16)
    return np.concatenate([high, high, low], axis=0)


def twiddles(length, taps):
    m = np.arange(LANES)
    rows = []
    for k in KEPT:
        angle = 2.0 * np.pi * k * m / length
        row = [np.cos(angle), -np.sin(angle)]
        weight = 1.0 if k in (0, RADIX * RADIX // 2) else 2.0
        row += [weight * np.cos(angle), weight * np.sin(angle)]
        for piece in range(taps // LANES):
            shifted = 2.0 * np.pi * k * (m + LANES * piece) / length
            row += [np.cos(shifted), -np.sin(shifted)]
        rows.append(np.stack(row))
    return np.stack(rows).astype(np.float32)


def cadd(a, b):
    return (a[0] + b[0], a[1] + b[1])


def csub(a, b):
    return (a[0] - b[0], a[1] - b[1])


def turn(a, num, den):
    num %= den
    if num == 0:
        return a
    if 4 * num == den:
        return (-a[1], a[0])
    if 2 * num == den:
        return (-a[0], -a[1])
    if 4 * num == 3 * den:
        return (a[1], -a[0])
    c, s = math.cos(2 * math.pi * num / den), math.sin(2 * math.pi * num / den)
    return (a[0] * c - a[1] * s, a[0] * s + a[1] * c)


def fourier(items, sign):
    n = len(items)
    if n == 1:
        return items
    even, odd = fourier(items[0::2], sign), fourier(items[1::2], sign)
    turned = [turn(o, sign * k, n) for k, o in enumerate(odd)]
    return [cadd(e, t) for e, t in zip(even, turned)] + [csub(e, t) for e, t in zip(even, turned)]


def real_eight(v):
    h = math.sqrt(0.5)
    s0, d0, s1, d1 = v[0] + v[4], v[0] - v[4], v[1] + v[5], v[1] - v[5]
    s2, d2, s3, d3 = v[2] + v[6], v[2] - v[6], v[3] + v[7], v[3] - v[7]
    p, q = s0 + s2, s1 + s3
    r, t = (d1 - d3) * h, (d1 + d3) * h
    return [p + q, (d0 + r, -(d2 + t)), (s0 - s2, s3 - s1), (d0 - r, d2 - t), p - q]


def eight_real(u0, u1, u2, u3, u4):
    h = math.sqrt(0.5)
    p, q = u0 + u4, u0 - u4
    e = [p + u2[0], q - u2[1], p - u2[0], q + u2[1]]
    f, g = u1[0] - u3[0], u1[1] + u3[1]
    o = [u1[0] + u3[0], (f - g) * h, u3[1] - u1[1], -(f + g) * h]
    return [a + b for a, b in zip(e, o)] + [a - b for a, b in zip(e, o)]


def put_split(ref, base, re, im):
    rows = pl.ds(base, ROWS)
    for part, value in enumerate((re, im)):
        high = value.astype(jnp.bfloat16)
        low = (value - high.astype(jnp.float32)).astype(jnp.bfloat16)
        at = part * LANES
        ref[rows, at : at + LANES] = high
        ref[rows, 2 * LANES + at : 2 * LANES + at + LANES] = low
        ref[rows, 4 * LANES + at : 4 * LANES + at + LANES] = high


def deconvolve(read, write, wave, floor, fwd_ref, inv_ref, tw_ref, mid_ref, cut_ref, spec_ref):
    half, wide = RADIX // 2, RADIX * RADIX
    for j2 in range(RADIX):
        out = real_eight([read(RADIX * j1 + j2) for j1 in range(RADIX)])
        mid_ref[2 * j2] = out[0]
        mid_ref[2 * j2 + 1] = out[half]
        for a in range(1, half):
            mid_ref[2 * RADIX * a + 2 * j2] = out[a][0]
            mid_ref[2 * RADIX * a + 2 * j2 + 1] = out[a][1]

    def emit(k, value):
        s = SLOT[k]
        c, n = tw_ref[s, 0:1, :], tw_ref[s, 1:2, :]
        put_split(cut_ref, s * ROWS, value[0] * c - value[1] * n, value[0] * n + value[1] * c)

    zero = real_eight([mid_ref[2 * j2] for j2 in range(RADIX)])
    c, n = tw_ref[0, 0:1, :], tw_ref[0, 1:2, :]
    for b in range(half + 1):
        s = SLOT[RADIX * b]
        c, n = tw_ref[s, 0:1, :], tw_ref[s, 1:2, :]
        if b in (0, half):
            put_split(cut_ref, s * ROWS, zero[b] * c, zero[b] * n)
        else:
            emit(RADIX * b, zero[b])
    for a in range(1, half):
        base = 2 * RADIX * a
        items = [turn((mid_ref[base + 2 * j2], mid_ref[base + 2 * j2 + 1]), -a * j2, wide) for j2 in range(RADIX)]
        for b, value in enumerate(fourier(items, -1)):
            emit(a + RADIX * b, value)
    four = [mid_ref[2 * j2 + 1] for j2 in range(RADIX)]
    for b in range(half):
        k = half + RADIX * b
        re, im = four[0], None
        for j2 in range(1, RADIX):
            angle = 2 * math.pi * (k * j2 % wide) / wide
            re = re + four[j2] * math.cos(angle)
            term = four[j2] * -math.sin(angle)
            im = term if im is None else im + term
        emit(k, (re, im))

    for s in range(KEEP):
        re = im = None
        for piece, taps in enumerate(wave):
            c, n = tw_ref[s, 4 + 2 * piece : 5 + 2 * piece, :], tw_ref[s, 5 + 2 * piece : 6 + 2 * piece, :]
            re = taps * c if re is None else re + taps * c
            im = taps * n if im is None else im + taps * n
        put_split(cut_ref, (KEEP + s) * ROWS, re, im)

    spec_ref[...] = jnp.dot(cut_ref[...], fwd_ref[...], preferred_element_type=jnp.float32)

    def apply(s, carry):
        at = pl.multiple_of(s * ROWS, ROWS)
        other = pl.multiple_of((KEEP + s) * ROWS, ROWS)
        xr, xi = spec_ref[pl.ds(at, ROWS), 0:LANES], spec_ref[pl.ds(at, ROWS), LANES:]
        hr, hi = spec_ref[pl.ds(other, ROWS), 0:LANES], spec_ref[pl.ds(other, ROWS), LANES:]
        scale = 1.0 / (hr * hr + hi * hi + floor)
        put_split(cut_ref, at, (xr * hr + xi * hi) * scale, (xi * hr - xr * hi) * scale)
        return carry

    lax.fori_loop(0, KEEP, apply, 0, unroll=3)
    rows = KEEP * ROWS
    spec_ref[0:rows] = jnp.dot(cut_ref[0:rows], inv_ref[...], preferred_element_type=jnp.float32)

    def fetch(k):
        s = SLOT[k]
        re, im = spec_ref[s * ROWS : (s + 1) * ROWS, 0:LANES], spec_ref[s * ROWS : (s + 1) * ROWS, LANES:]
        c, n = tw_ref[s, 2:3, :], tw_ref[s, 3:4, :]
        if k in (0, wide // 2):
            return re * c - im * n
        return (re * c - im * n, re * n + im * c)

    for a in range(1, half):
        base = 2 * RADIX * a
        for j2, value in enumerate(fourier([fetch(a + RADIX * b) for b in range(RADIX)], 1)):
            value = turn(value, a * j2, wide)
            mid_ref[base + 2 * j2] = value[0]
            mid_ref[base + 2 * j2 + 1] = value[1]
    for j2, value in enumerate(eight_real(*[fetch(RADIX * b) for b in range(half + 1)])):
        mid_ref[2 * j2] = value
    four = [fetch(half + RADIX * b) for b in range(half)]
    for j2 in range(RADIX):
        total = None
        for b, value in enumerate(four):
            angle = 2 * math.pi * ((half + RADIX * b) * j2 % wide) / wide
            term = value[0] * math.cos(angle)
            if j2:
                term = term - value[1] * math.sin(angle)
            total = term if total is None else total + term
        mid_ref[2 * j2 + 1] = total
    for j2 in range(RADIX):
        parts = [mid_ref[2 * j2]]
        for a in range(1, half):
            base = 2 * RADIX * a
            parts.append((mid_ref[base + 2 * j2], mid_ref[base + 2 * j2 + 1]))
        parts.append(mid_ref[2 * j2 + 1])
        for j1, value in enumerate(eight_real(*parts)):
            write(RADIX * j1 + j2, value)


def block_kernel(taps, x_ref, w_ref, fwd_ref, inv_ref, tw_ref, o_ref, mid_ref, cut_ref, spec_ref):
    def read(j):
        return x_ref[:, j * LANES : (j + 1) * LANES]

    def write(j, value):
        o_ref[:, j * LANES : (j + 1) * LANES] = value

    wave = [w_ref[:, p * LANES : (p + 1) * LANES] for p in range(taps // LANES)]
    deconvolve(read, write, wave, w_ref[:, taps : taps + LANES], fwd_ref, inv_ref, tw_ref, mid_ref, cut_ref, spec_ref)


def tables(length, taps):
    return (
        jnp.asarray(lane_matrix(-1.0, 1.0)),
        jnp.asarray(lane_matrix(1.0, 1.0 / length)),
        jnp.asarray(twiddles(length, taps)),
    )


def scratch():
    return [
        pltpu.VMEM((RADIX * RADIX, ROWS, LANES), jnp.float32),
        pltpu.VMEM((2 * KEEP * ROWS, 6 * LANES), jnp.bfloat16),
        pltpu.VMEM((2 * KEEP * ROWS, 2 * LANES), jnp.float32),
    ]


def local(raw_traces, filter_index, channel_order, wavelets, damping):
    rows, length = raw_traces.shape
    taps = wavelets.shape[1]
    n = lax.axis_size("traces")
    each = rows // n
    floor = damping * (jnp.sum(wavelets * wavelets, axis=1) + 1e-6)
    packed = jnp.concatenate([wavelets, jnp.broadcast_to(floor[:, None], (floor.shape[0], LANES))], axis=1)
    bank = lax.all_gather(packed, "traces", axis=0, tiled=True)
    came = lax.all_to_all(raw_traces.reshape(n, each, length), "traces", 0, 0, tiled=True).reshape(rows, length)
    picks = lax.all_to_all(filter_index.reshape(n, each), "traces", 0, 0, tiled=True).reshape(rows)
    chosen = jnp.take(bank, picks, axis=0)
    fwd, inv, tw = tables(length, taps)
    whole = lambda a: pl.BlockSpec(a.shape, lambda i: (0,) * a.ndim)
    result = pl.pallas_call(
        functools.partial(block_kernel, taps),
        grid=(rows // ROWS,),
        out_shape=jax.ShapeDtypeStruct((rows, length), jnp.float32),
        in_specs=[
            pl.BlockSpec((ROWS, length), lambda i: (i, 0)),
            pl.BlockSpec((ROWS, taps + LANES), lambda i: (i, 0)),
            whole(fwd),
            whole(inv),
            whole(tw),
        ],
        out_specs=pl.BlockSpec((ROWS, length), lambda i: (i, 0)),
        scratch_shapes=scratch(),
        compiler_params=pltpu.CompilerParams(vmem_limit_bytes=40 * 1024 * 1024),
    )(came, chosen, fwd, inv, tw)
    source = (channel_order % n) * each + channel_order // n
    return jnp.take(result, source, axis=0)


def solution(mesh):
    placed = (
        P(("groups", "traces"), None),
        P(("groups", "traces")),
        P("groups"),
        P("traces", None),
        P("traces"),
    )
    return jax.shard_map(
        local, mesh=mesh, in_specs=placed, out_specs=P(("groups", "traces"), None), check_vma=False
    )
```

```python
import functools
import math

import jax
import jax.numpy as jnp
import numpy as np
from jax import lax
from jax.experimental import pallas as pl
from jax.experimental.pallas import tpu as pltpu
from jax.sharding import PartitionSpec as P

LANES = 128
RADIX = 8
ROWS = 16
SUBLANES = 8

KEPT = (
    [RADIX * b for b in range(RADIX // 2 + 1)]
    + [a + RADIX * b for a in range(1, RADIX // 2) for b in range(RADIX)]
    + [RADIX // 2 + RADIX * b for b in range(RADIX // 2)]
)
SLOT = {k: s for s, k in enumerate(KEPT)}
KEEP = len(KEPT)


def lane_matrix(sign, scale):
    ids = np.arange(LANES)
    angle = 2.0 * np.pi * (np.outer(ids, ids) % LANES) / LANES
    c, s = np.cos(angle) * scale, sign * np.sin(angle) * scale
    full = np.block([[c, s], [-s, c]])
    import ml_dtypes

    high = full.astype(np.float32).astype(ml_dtypes.bfloat16)
    low = (full.astype(np.float32) - high.astype(np.float32)).astype(ml_dtypes.bfloat16)
    return np.concatenate([high, high, low], axis=0)


def twiddles(length, taps):
    m = np.arange(LANES)
    rows = []
    for k in KEPT:
        angle = 2.0 * np.pi * k * m / length
        row = [np.cos(angle), -np.sin(angle)]
        weight = 1.0 if k in (0, RADIX * RADIX // 2) else 2.0
        row += [weight * np.cos(angle), weight * np.sin(angle)]
        for piece in range(taps // LANES):
            shifted = 2.0 * np.pi * k * (m + LANES * piece) / length
            row += [np.cos(shifted), -np.sin(shifted)]
        rows.append(np.stack(row))
    return np.stack(rows).astype(np.float32)


def cadd(a, b):
    return (a[0] + b[0], a[1] + b[1])


def csub(a, b):
    return (a[0] - b[0], a[1] - b[1])


def turn(a, num, den):
    num %= den
    if num == 0:
        return a
    if 4 * num == den:
        return (-a[1], a[0])
    if 2 * num == den:
        return (-a[0], -a[1])
    if 4 * num == 3 * den:
        return (a[1], -a[0])
    c, s = math.cos(2 * math.pi * num / den), math.sin(2 * math.pi * num / den)
    return (a[0] * c - a[1] * s, a[0] * s + a[1] * c)


def fourier(items, sign):
    n = len(items)
    if n == 1:
        return items
    even, odd = fourier(items[0::2], sign), fourier(items[1::2], sign)
    turned = [turn(o, sign * k, n) for k, o in enumerate(odd)]
    return [cadd(e, t) for e, t in zip(even, turned)] + [csub(e, t) for e, t in zip(even, turned)]


def real_eight(v):
    h = math.sqrt(0.5)
    s0, d0, s1, d1 = v[0] + v[4], v[0] - v[4], v[1] + v[5], v[1] - v[5]
    s2, d2, s3, d3 = v[2] + v[6], v[2] - v[6], v[3] + v[7], v[3] - v[7]
    p, q = s0 + s2, s1 + s3
    r, t = (d1 - d3) * h, (d1 + d3) * h
    return [p + q, (d0 + r, -(d2 + t)), (s0 - s2, s3 - s1), (d0 - r, d2 - t), p - q]


def eight_real(u0, u1, u2, u3, u4):
    h = math.sqrt(0.5)
    p, q = u0 + u4, u0 - u4
    e = [p + u2[0], q - u2[1], p - u2[0], q + u2[1]]
    f, g = u1[0] - u3[0], u1[1] + u3[1]
    o = [u1[0] + u3[0], (f - g) * h, u3[1] - u1[1], -(f + g) * h]
    return [a + b for a, b in zip(e, o)] + [a - b for a, b in zip(e, o)]


def put_split(ref, base, re, im):
    rows = pl.ds(base, ROWS)
    for part, value in enumerate((re, im)):
        high = value.astype(jnp.bfloat16)
        low = (value - high.astype(jnp.float32)).astype(jnp.bfloat16)
        at = part * LANES
        ref[rows, at : at + LANES] = high
        ref[rows, 2 * LANES + at : 2 * LANES + at + LANES] = low
        ref[rows, 4 * LANES + at : 4 * LANES + at + LANES] = high


def deconvolve(read, write, wave, floor, fwd_ref, inv_ref, tw_ref, mid_ref, cut_ref, spec_ref):
    half, wide = RADIX // 2, RADIX * RADIX
    for j2 in range(RADIX):
        out = real_eight([read(RADIX * j1 + j2) for j1 in range(RADIX)])
        mid_ref[2 * j2] = out[0]
        mid_ref[2 * j2 + 1] = out[half]
        for a in range(1, half):
            mid_ref[2 * RADIX * a + 2 * j2] = out[a][0]
            mid_ref[2 * RADIX * a + 2 * j2 + 1] = out[a][1]

    def emit(k, value):
        s = SLOT[k]
        c, n = tw_ref[s, 0:1, :], tw_ref[s, 1:2, :]
        put_split(cut_ref, s * ROWS, value[0] * c - value[1] * n, value[0] * n + value[1] * c)

    zero = real_eight([mid_ref[2 * j2] for j2 in range(RADIX)])
    c, n = tw_ref[0, 0:1, :], tw_ref[0, 1:2, :]
    for b in range(half + 1):
        s = SLOT[RADIX * b]
        c, n = tw_ref[s, 0:1, :], tw_ref[s, 1:2, :]
        if b in (0, half):
            put_split(cut_ref, s * ROWS, zero[b] * c, zero[b] * n)
        else:
            emit(RADIX * b, zero[b])
    for a in range(1, half):
        base = 2 * RADIX * a
        items = [turn((mid_ref[base + 2 * j2], mid_ref[base + 2 * j2 + 1]), -a * j2, wide) for j2 in range(RADIX)]
        for b, value in enumerate(fourier(items, -1)):
            emit(a + RADIX * b, value)
    four = [mid_ref[2 * j2 + 1] for j2 in range(RADIX)]
    for b in range(half):
        k = half + RADIX * b
        re, im = four[0], None
        for j2 in range(1, RADIX):
            angle = 2 * math.pi * (k * j2 % wide) / wide
            re = re + four[j2] * math.cos(angle)
            term = four[j2] * -math.sin(angle)
            im = term if im is None else im + term
        emit(k, (re, im))

    for s in range(KEEP):
        re = im = None
        for piece, taps in enumerate(wave):
            c, n = tw_ref[s, 4 + 2 * piece : 5 + 2 * piece, :], tw_ref[s, 5 + 2 * piece : 6 + 2 * piece, :]
            re = taps * c if re is None else re + taps * c
            im = taps * n if im is None else im + taps * n
        put_split(cut_ref, (KEEP + s) * ROWS, re, im)

    spec_ref[...] = jnp.dot(cut_ref[...], fwd_ref[...], preferred_element_type=jnp.float32)

    def apply(s, carry):
        at = pl.multiple_of(s * ROWS, ROWS)
        other = pl.multiple_of((KEEP + s) * ROWS, ROWS)
        xr, xi = spec_ref[pl.ds(at, ROWS), 0:LANES], spec_ref[pl.ds(at, ROWS), LANES:]
        hr, hi = spec_ref[pl.ds(other, ROWS), 0:LANES], spec_ref[pl.ds(other, ROWS), LANES:]
        scale = 1.0 / (hr * hr + hi * hi + floor)
        put_split(cut_ref, at, (xr * hr + xi * hi) * scale, (xi * hr - xr * hi) * scale)
        return carry

    lax.fori_loop(0, KEEP, apply, 0, unroll=3)
    rows = KEEP * ROWS
    spec_ref[0:rows] = jnp.dot(cut_ref[0:rows], inv_ref[...], preferred_element_type=jnp.float32)

    def fetch(k):
        s = SLOT[k]
        re, im = spec_ref[s * ROWS : (s + 1) * ROWS, 0:LANES], spec_ref[s * ROWS : (s + 1) * ROWS, LANES:]
        c, n = tw_ref[s, 2:3, :], tw_ref[s, 3:4, :]
        if k in (0, wide // 2):
            return re * c - im * n
        return (re * c - im * n, re * n + im * c)

    for a in range(1, half):
        base = 2 * RADIX * a
        for j2, value in enumerate(fourier([fetch(a + RADIX * b) for b in range(RADIX)], 1)):
            value = turn(value, a * j2, wide)
            mid_ref[base + 2 * j2] = value[0]
            mid_ref[base + 2 * j2 + 1] = value[1]
    for j2, value in enumerate(eight_real(*[fetch(RADIX * b) for b in range(half + 1)])):
        mid_ref[2 * j2] = value
    four = [fetch(half + RADIX * b) for b in range(half)]
    for j2 in range(RADIX):
        total = None
        for b, value in enumerate(four):
            angle = 2 * math.pi * ((half + RADIX * b) * j2 % wide) / wide
            term = value[0] * math.cos(angle)
            if j2:
                term = term - value[1] * math.sin(angle)
            total = term if total is None else total + term
        mid_ref[2 * j2 + 1] = total
    for j2 in range(RADIX):
        parts = [mid_ref[2 * j2]]
        for a in range(1, half):
            base = 2 * RADIX * a
            parts.append((mid_ref[base + 2 * j2], mid_ref[base + 2 * j2 + 1]))
        parts.append(mid_ref[2 * j2 + 1])
        for j1, value in enumerate(eight_real(*parts)):
            write(RADIX * j1 + j2, value)


def slabs(ref, lead):
    def at(j):
        return lead + (slice(None), slice(j * LANES, (j + 1) * LANES))

    def read(j):
        value = ref[at(j)]
        return value.reshape(ROWS, LANES)

    def write(j, value):
        ref[at(j)] = value.reshape(ref[at(j)].shape)

    return read, write


def block_kernel(taps, lead, x_ref, w_ref, fwd_ref, inv_ref, tw_ref, o_ref, mid_ref, cut_ref, spec_ref):
    read, _ = slabs(x_ref, lead)
    _, write = slabs(o_ref, (slice(None),) * (len(o_ref.shape) - 2))
    wave = [w_ref[:, p * LANES : (p + 1) * LANES] for p in range(taps // LANES)]
    deconvolve(read, write, wave, w_ref[:, taps : taps + LANES], fwd_ref, inv_ref, tw_ref, mid_ref, cut_ref, spec_ref)


def place_kernel(taps, row_ref, x_ref, w_ref, fwd_ref, inv_ref, tw_ref, o_ref, mid_ref, cut_ref, spec_ref, res_ref, sems):
    step, steps = pl.program_id(0), pl.num_programs(0)
    slot = lax.rem(step, 2)

    def rows_of(at, slot, act):
        for r in range(ROWS):
            copy = pltpu.make_async_copy(
                res_ref.at[slot, pl.ds(r, 1)], o_ref.at[pl.ds(row_ref[at * ROWS + r], 1)], sems.at[slot, r]
            )
            act(copy)

    @pl.when(step >= 2)
    def _():
        rows_of(step - 2, slot, lambda copy: copy.wait())

    read, _ = slabs(x_ref, (slice(None),) * (len(x_ref.shape) - 2))

    def write(j, value):
        res_ref[slot, :, j * LANES : (j + 1) * LANES] = value

    wave = [w_ref[:, p * LANES : (p + 1) * LANES] for p in range(taps // LANES)]
    deconvolve(read, write, wave, w_ref[:, taps : taps + LANES], fwd_ref, inv_ref, tw_ref, mid_ref, cut_ref, spec_ref)
    rows_of(step, slot, lambda copy: copy.start())

    @pl.when(step == steps - 1)
    def _():
        @pl.when(step >= 1)
        def _():
            rows_of(step - 1, 1 - slot, lambda copy: copy.wait())

        rows_of(step, slot, lambda copy: copy.wait())


def settle_kernel(row_ref, came_ref, filled_ref, o_ref, held_ref, in_sems, out_sems):
    del filled_ref
    blocks, rows, _ = came_ref.shape

    def take(d):
        return pltpu.make_async_copy(came_ref.at[d], held_ref.at[d], in_sems.at[d])

    def put(d, r):
        return pltpu.make_async_copy(
            held_ref.at[d, pl.ds(r, 1)], o_ref.at[pl.ds(row_ref[d * rows + r], 1)], out_sems.at[d, r]
        )

    for d in range(blocks):
        take(d).start()

    def send(d, carry):
        take(d).wait()
        for r in range(rows):
            put(d, r).start()
        return carry

    lax.fori_loop(0, blocks, send, 0)

    def finish(d, carry):
        for r in range(rows):
            put(d, r).wait()
        return carry

    lax.fori_loop(0, blocks, finish, 0)


def tables(length, taps):
    return (
        jnp.asarray(lane_matrix(-1.0, 1.0)),
        jnp.asarray(lane_matrix(1.0, 1.0 / length)),
        jnp.asarray(twiddles(length, taps)),
    )


def scratch():
    return [
        pltpu.VMEM((RADIX * RADIX, ROWS, LANES), jnp.float32),
        pltpu.VMEM((2 * KEEP * ROWS, 6 * LANES), jnp.bfloat16),
        pltpu.VMEM((2 * KEEP * ROWS, 2 * LANES), jnp.float32),
    ]


def local(raw_traces, filter_index, channel_order, wavelets, damping):
    rows, length = raw_traces.shape
    own, taps = wavelets.shape
    n = lax.axis_size("traces")
    me = lax.axis_index("traces")
    each = rows // n
    floor = damping * (jnp.sum(wavelets * wavelets, axis=1) + 1e-6)
    picks = filter_index.reshape(own, rows // own).astype(jnp.float32)
    packed = lax.all_gather(jnp.concatenate([wavelets, floor[:, None], picks], axis=1), "traces", axis=0, tiled=True)
    all_picks = packed[:, taps + 1 :].reshape(n, n, each).astype(jnp.int32)
    came_picks = lax.dynamic_index_in_dim(all_picks, me, 1, keepdims=False)
    bank = jnp.concatenate([packed[:, :taps], jnp.broadcast_to(packed[:, taps : taps + 1], (own * n, LANES))], axis=1)
    fwd, inv, tw = tables(length, taps)
    whole = lambda a: pl.BlockSpec(a.shape, lambda i, *_: (0,) * a.ndim)
    fixed = [pl.BlockSpec((ROWS, taps + LANES), lambda i, *_: (i, 0)), whole(fwd), whole(inv), whole(tw)]
    params = pltpu.CompilerParams(vmem_limit_bytes=48 * 1024 * 1024)
    places = (jnp.arange(each)[None, :] * n + jnp.arange(n)[:, None]).reshape(-1)

    if each % (2 * SUBLANES):
        came = lax.all_to_all(raw_traces.reshape(n, each, length), "traces", 0, 0, tiled=True).reshape(rows, length)
        result = pl.pallas_call(
            functools.partial(block_kernel, taps, ()),
            grid=(rows // ROWS,),
            out_shape=jax.ShapeDtypeStruct((rows, length), jnp.float32),
            in_specs=[pl.BlockSpec((ROWS, length), lambda i: (i, 0))] + fixed,
            out_specs=pl.BlockSpec((ROWS, length), lambda i: (i, 0)),
            scratch_shapes=scratch(),
            compiler_params=params,
        )(came, jnp.take(bank, came_picks.reshape(-1), axis=0), fwd, inv, tw)
        return jnp.take(result, (channel_order % n) * each + channel_order // n, axis=0)

    hits = channel_order[None, :] == places[:, None]
    row_of = jnp.sum(jnp.where(hits, jnp.arange(rows)[None, :], 0), axis=1).reshape(n, 2, each // 2)
    part = each // 2
    group = ROWS // part if part < ROWS else 1
    split = raw_traces.reshape(n, 2, part, length)
    steps = n // group
    flops = pl.CostEstimate(flops=steps * ROWS * length * 1500, bytes_accessed=8 * steps * ROWS * length, transcendentals=0)

    came_raw = lax.all_to_all(split[:, 0], "traces", 0, 0, tiled=True)
    own_rows = filter_index.reshape(n, 2, part)[:, 1].reshape(-1)
    done_here = pl.pallas_call(
        functools.partial(block_kernel, taps, (slice(None), 0)),
        grid=(steps,),
        out_shape=jax.ShapeDtypeStruct((n, part, length), jnp.float32),
        in_specs=[pl.BlockSpec((group, 1, part, length), lambda i: (i, 1, 0, 0))] + fixed,
        out_specs=pl.BlockSpec((group, part, length), lambda i: (i, 0, 0)),
        scratch_shapes=scratch(),
        compiler_params=params,
        cost_estimate=flops,
    )(split, jnp.take(bank, own_rows, axis=0), fwd, inv, tw)
    came_done = lax.all_to_all(done_here, "traces", 0, 0, tiled=True)
    came_rows = came_picks[:, :part].reshape(-1)
    filled = pl.pallas_call(
        functools.partial(place_kernel, taps),
        grid_spec=pltpu.PrefetchScalarGridSpec(
            num_scalar_prefetch=1,
            grid=(steps,),
            in_specs=[pl.BlockSpec((group, part, length), lambda i, *_: (i, 0, 0))] + fixed,
            out_specs=pl.BlockSpec(memory_space=pl.ANY),
            scratch_shapes=scratch()
            + [pltpu.VMEM((2, ROWS, length), jnp.float32), pltpu.SemaphoreType.DMA((2, ROWS))],
        ),
        out_shape=jax.ShapeDtypeStruct((rows, length), jnp.float32),
        compiler_params=params,
        cost_estimate=flops,
    )(row_of[:, 0].reshape(-1), came_raw, jnp.take(bank, came_rows, axis=0), fwd, inv, tw)
    return pl.pallas_call(
        settle_kernel,
        in_specs=[pl.BlockSpec(memory_space=pltpu.SMEM)] + [pl.BlockSpec(memory_space=pl.ANY)] * 2,
        out_specs=pl.BlockSpec(memory_space=pl.ANY),
        out_shape=jax.ShapeDtypeStruct((rows, length), jnp.float32),
        scratch_shapes=[
            pltpu.VMEM((n, part, length), jnp.float32),
            pltpu.SemaphoreType.DMA((n,)),
            pltpu.SemaphoreType.DMA((n, part)),
        ],
        input_output_aliases={2: 0},
        compiler_params=params,
    )(row_of[:, 1].reshape(-1), came_done, filled)


def solution(mesh):
    placed = (
        P(("groups", "traces"), None),
        P(("groups", "traces")),
        P("groups"),
        P("traces", None),
        P("traces"),
    )
    return jax.shard_map(
        local, mesh=mesh, in_specs=placed, out_specs=P(("groups", "traces"), None), check_vma=False
    )
```

```python
import functools
import math

import jax
import jax.numpy as jnp
import numpy as np
from jax import lax
from jax.experimental import pallas as pl
from jax.experimental.pallas import tpu as pltpu
from jax.sharding import PartitionSpec as P

LANES = 128
RADIX = 8
ROWS = 16
SUBLANES = 8

KEPT = (
    [RADIX * b for b in range(RADIX // 2 + 1)]
    + [a + RADIX * b for a in range(1, RADIX // 2) for b in range(RADIX)]
    + [RADIX // 2 + RADIX * b for b in range(RADIX // 2)]
)
SLOT = {k: s for s, k in enumerate(KEPT)}
KEEP = len(KEPT)


def lane_matrix(sign, scale):
    ids = np.arange(LANES)
    angle = 2.0 * np.pi * (np.outer(ids, ids) % LANES) / LANES
    c, s = np.cos(angle) * scale, sign * np.sin(angle) * scale
    full = np.block([[c, s], [-s, c]])
    import ml_dtypes

    high = full.astype(np.float32).astype(ml_dtypes.bfloat16)
    low = (full.astype(np.float32) - high.astype(np.float32)).astype(ml_dtypes.bfloat16)
    return np.concatenate([high, high, low], axis=0)


def twiddles(length, taps):
    m = np.arange(LANES)
    rows = []
    for k in KEPT:
        angle = 2.0 * np.pi * k * m / length
        row = [np.cos(angle), -np.sin(angle)]
        weight = 1.0 if k in (0, RADIX * RADIX // 2) else 2.0
        row += [weight * np.cos(angle), weight * np.sin(angle)]
        for piece in range(taps // LANES):
            shifted = 2.0 * np.pi * k * (m + LANES * piece) / length
            row += [np.cos(shifted), -np.sin(shifted)]
        rows.append(np.stack(row))
    return np.stack(rows).astype(np.float32)


def cadd(a, b):
    return (a[0] + b[0], a[1] + b[1])


def csub(a, b):
    return (a[0] - b[0], a[1] - b[1])


def turn(a, num, den):
    num %= den
    if num == 0:
        return a
    if 4 * num == den:
        return (-a[1], a[0])
    if 2 * num == den:
        return (-a[0], -a[1])
    if 4 * num == 3 * den:
        return (a[1], -a[0])
    c, s = math.cos(2 * math.pi * num / den), math.sin(2 * math.pi * num / den)
    return (a[0] * c - a[1] * s, a[0] * s + a[1] * c)


def fourier(items, sign):
    n = len(items)
    if n == 1:
        return items
    even, odd = fourier(items[0::2], sign), fourier(items[1::2], sign)
    turned = [turn(o, sign * k, n) for k, o in enumerate(odd)]
    return [cadd(e, t) for e, t in zip(even, turned)] + [csub(e, t) for e, t in zip(even, turned)]


def real_eight(v):
    h = math.sqrt(0.5)
    s0, d0, s1, d1 = v[0] + v[4], v[0] - v[4], v[1] + v[5], v[1] - v[5]
    s2, d2, s3, d3 = v[2] + v[6], v[2] - v[6], v[3] + v[7], v[3] - v[7]
    p, q = s0 + s2, s1 + s3
    r, t = (d1 - d3) * h, (d1 + d3) * h
    return [p + q, (d0 + r, -(d2 + t)), (s0 - s2, s3 - s1), (d0 - r, d2 - t), p - q]


def eight_real(u0, u1, u2, u3, u4):
    h = math.sqrt(0.5)
    p, q = u0 + u4, u0 - u4
    e = [p + u2[0], q - u2[1], p - u2[0], q + u2[1]]
    f, g = u1[0] - u3[0], u1[1] + u3[1]
    o = [u1[0] + u3[0], (f - g) * h, u3[1] - u1[1], -(f + g) * h]
    return [a + b for a, b in zip(e, o)] + [a - b for a, b in zip(e, o)]


def put_split(ref, base, re, im):
    rows = pl.ds(base, ROWS)
    for part, value in enumerate((re, im)):
        high = value.astype(jnp.bfloat16)
        low = (value - high.astype(jnp.float32)).astype(jnp.bfloat16)
        at = part * LANES
        ref[rows, at : at + LANES] = high
        ref[rows, 2 * LANES + at : 2 * LANES + at + LANES] = low
        ref[rows, 4 * LANES + at : 4 * LANES + at + LANES] = high


def deconvolve(read, write, wave, floor, fwd_ref, inv_ref, tw_ref, mid_ref, cut_ref, spec_ref):
    half, wide = RADIX // 2, RADIX * RADIX
    for j2 in range(RADIX):
        out = real_eight([read(RADIX * j1 + j2) for j1 in range(RADIX)])
        mid_ref[2 * j2] = out[0]
        mid_ref[2 * j2 + 1] = out[half]
        for a in range(1, half):
            mid_ref[2 * RADIX * a + 2 * j2] = out[a][0]
            mid_ref[2 * RADIX * a + 2 * j2 + 1] = out[a][1]

    def emit(k, value):
        s = SLOT[k]
        c, n = tw_ref[s, 0:1, :], tw_ref[s, 1:2, :]
        put_split(cut_ref, s * ROWS, value[0] * c - value[1] * n, value[0] * n + value[1] * c)

    zero = real_eight([mid_ref[2 * j2] for j2 in range(RADIX)])
    c, n = tw_ref[0, 0:1, :], tw_ref[0, 1:2, :]
    for b in range(half + 1):
        s = SLOT[RADIX * b]
        c, n = tw_ref[s, 0:1, :], tw_ref[s, 1:2, :]
        if b in (0, half):
            put_split(cut_ref, s * ROWS, zero[b] * c, zero[b] * n)
        else:
            emit(RADIX * b, zero[b])
    for a in range(1, half):
        base = 2 * RADIX * a
        items = [turn((mid_ref[base + 2 * j2], mid_ref[base + 2 * j2 + 1]), -a * j2, wide) for j2 in range(RADIX)]
        for b, value in enumerate(fourier(items, -1)):
            emit(a + RADIX * b, value)
    four = [mid_ref[2 * j2 + 1] for j2 in range(RADIX)]
    for b in range(half):
        k = half + RADIX * b
        re, im = four[0], None
        for j2 in range(1, RADIX):
            angle = 2 * math.pi * (k * j2 % wide) / wide
            re = re + four[j2] * math.cos(angle)
            term = four[j2] * -math.sin(angle)
            im = term if im is None else im + term
        emit(k, (re, im))

    for s in range(KEEP):
        re = im = None
        for piece, taps in enumerate(wave):
            c, n = tw_ref[s, 4 + 2 * piece : 5 + 2 * piece, :], tw_ref[s, 5 + 2 * piece : 6 + 2 * piece, :]
            re = taps * c if re is None else re + taps * c
            im = taps * n if im is None else im + taps * n
        put_split(cut_ref, (KEEP + s) * ROWS, re, im)

    spec_ref[...] = jnp.dot(cut_ref[...], fwd_ref[...], preferred_element_type=jnp.float32)

    def apply(s, carry):
        at = pl.multiple_of(s * ROWS, ROWS)
        other = pl.multiple_of((KEEP + s) * ROWS, ROWS)
        xr, xi = spec_ref[pl.ds(at, ROWS), 0:LANES], spec_ref[pl.ds(at, ROWS), LANES:]
        hr, hi = spec_ref[pl.ds(other, ROWS), 0:LANES], spec_ref[pl.ds(other, ROWS), LANES:]
        scale = 1.0 / (hr * hr + hi * hi + floor)
        put_split(cut_ref, at, (xr * hr + xi * hi) * scale, (xi * hr - xr * hi) * scale)
        return carry

    lax.fori_loop(0, KEEP, apply, 0, unroll=3)
    rows = KEEP * ROWS
    spec_ref[0:rows] = jnp.dot(cut_ref[0:rows], inv_ref[...], preferred_element_type=jnp.float32)

    def fetch(k):
        s = SLOT[k]
        re, im = spec_ref[s * ROWS : (s + 1) * ROWS, 0:LANES], spec_ref[s * ROWS : (s + 1) * ROWS, LANES:]
        c, n = tw_ref[s, 2:3, :], tw_ref[s, 3:4, :]
        if k in (0, wide // 2):
            return re * c - im * n
        return (re * c - im * n, re * n + im * c)

    for a in range(1, half):
        base = 2 * RADIX * a
        for j2, value in enumerate(fourier([fetch(a + RADIX * b) for b in range(RADIX)], 1)):
            value = turn(value, a * j2, wide)
            mid_ref[base + 2 * j2] = value[0]
            mid_ref[base + 2 * j2 + 1] = value[1]
    for j2, value in enumerate(eight_real(*[fetch(RADIX * b) for b in range(half + 1)])):
        mid_ref[2 * j2] = value
    four = [fetch(half + RADIX * b) for b in range(half)]
    for j2 in range(RADIX):
        total = None
        for b, value in enumerate(four):
            angle = 2 * math.pi * ((half + RADIX * b) * j2 % wide) / wide
            term = value[0] * math.cos(angle)
            if j2:
                term = term - value[1] * math.sin(angle)
            total = term if total is None else total + term
        mid_ref[2 * j2 + 1] = total
    for j2 in range(RADIX):
        parts = [mid_ref[2 * j2]]
        for a in range(1, half):
            base = 2 * RADIX * a
            parts.append((mid_ref[base + 2 * j2], mid_ref[base + 2 * j2 + 1]))
        parts.append(mid_ref[2 * j2 + 1])
        for j1, value in enumerate(eight_real(*parts)):
            write(RADIX * j1 + j2, value)


def slabs(ref, lead):
    def at(j):
        return lead + (slice(None), slice(j * LANES, (j + 1) * LANES))

    def read(j):
        value = ref[at(j)]
        return value.reshape(ROWS, LANES)

    def write(j, value):
        ref[at(j)] = value.reshape(ref[at(j)].shape)

    return read, write


def block_kernel(taps, lead, x_ref, w_ref, fwd_ref, inv_ref, tw_ref, o_ref, mid_ref, cut_ref, spec_ref):
    read, _ = slabs(x_ref, lead)
    _, write = slabs(o_ref, (slice(None),) * (len(o_ref.shape) - 2))
    wave = [w_ref[:, p * LANES : (p + 1) * LANES] for p in range(taps // LANES)]
    deconvolve(read, write, wave, w_ref[:, taps : taps + LANES], fwd_ref, inv_ref, tw_ref, mid_ref, cut_ref, spec_ref)


def place_kernel(taps, row_ref, x_ref, w_ref, fwd_ref, inv_ref, tw_ref, o_ref, mid_ref, cut_ref, spec_ref, res_ref, sems):
    step, steps = pl.program_id(0), pl.num_programs(0)
    slot = lax.rem(step, 2)

    def rows_of(at, slot, act):
        for r in range(ROWS):
            copy = pltpu.make_async_copy(
                res_ref.at[slot, pl.ds(r, 1)], o_ref.at[pl.ds(row_ref[at * ROWS + r], 1)], sems.at[slot, r]
            )
            act(copy)

    @pl.when(step >= 2)
    def _():
        rows_of(step - 2, slot, lambda copy: copy.wait())

    read, _ = slabs(x_ref, (slice(None),) * (len(x_ref.shape) - 2))

    def write(j, value):
        res_ref[slot, :, j * LANES : (j + 1) * LANES] = value

    wave = [w_ref[:, p * LANES : (p + 1) * LANES] for p in range(taps // LANES)]
    deconvolve(read, write, wave, w_ref[:, taps : taps + LANES], fwd_ref, inv_ref, tw_ref, mid_ref, cut_ref, spec_ref)
    rows_of(step, slot, lambda copy: copy.start())

    @pl.when(step == steps - 1)
    def _():
        @pl.when(step >= 1)
        def _():
            rows_of(step - 1, 1 - slot, lambda copy: copy.wait())

        rows_of(step, slot, lambda copy: copy.wait())


def settle_kernel(row_ref, came_ref, filled_ref, o_ref, held_ref, in_sems, out_sems):
    del filled_ref
    blocks, rows, _ = came_ref.shape

    def take(d):
        return pltpu.make_async_copy(came_ref.at[d], held_ref.at[d], in_sems.at[d])

    def put(d, r):
        return pltpu.make_async_copy(
            held_ref.at[d, pl.ds(r, 1)], o_ref.at[pl.ds(row_ref[d * rows + r], 1)], out_sems.at[d, r]
        )

    for d in range(blocks):
        take(d).start()

    def send(d, carry):
        take(d).wait()
        for r in range(rows):
            put(d, r).start()
        return carry

    lax.fori_loop(0, blocks, send, 0)

    def finish(d, carry):
        for r in range(rows):
            put(d, r).wait()
        return carry

    lax.fori_loop(0, blocks, finish, 0)


def tables(length, taps):
    return (
        jnp.asarray(lane_matrix(-1.0, 1.0)),
        jnp.asarray(lane_matrix(1.0, 1.0 / length)),
        jnp.asarray(twiddles(length, taps)),
    )


def scratch():
    return [
        pltpu.VMEM((RADIX * RADIX, ROWS, LANES), jnp.float32),
        pltpu.VMEM((2 * KEEP * ROWS, 6 * LANES), jnp.bfloat16),
        pltpu.VMEM((2 * KEEP * ROWS, 2 * LANES), jnp.float32),
    ]


def local(raw_traces, filter_index, channel_order, wavelets, damping):
    rows, length = raw_traces.shape
    own, taps = wavelets.shape
    n = lax.axis_size("traces")
    me = lax.axis_index("traces")
    each = rows // n
    floor = damping * (jnp.sum(wavelets * wavelets, axis=1) + 1e-6)
    picks = filter_index.reshape(own, rows // own).astype(jnp.float32)
    packed = lax.all_gather(jnp.concatenate([wavelets, floor[:, None], picks], axis=1), "traces", axis=0, tiled=True)
    part = each // 2
    first = raw_traces.reshape(n, each, length)[:, :part]
    first, packed = lax.optimization_barrier((first, packed))
    all_picks = packed[:, taps + 1 :].reshape(n, n, each).astype(jnp.int32)
    came_picks = lax.dynamic_index_in_dim(all_picks, me, 1, keepdims=False)
    bank = jnp.concatenate([packed[:, :taps], jnp.broadcast_to(packed[:, taps : taps + 1], (own * n, LANES))], axis=1)
    fwd, inv, tw = tables(length, taps)
    whole = lambda a: pl.BlockSpec(a.shape, lambda i, *_: (0,) * a.ndim)
    fixed = [pl.BlockSpec((ROWS, taps + LANES), lambda i, *_: (i, 0)), whole(fwd), whole(inv), whole(tw)]
    params = pltpu.CompilerParams(vmem_limit_bytes=48 * 1024 * 1024)
    places = (jnp.arange(each)[None, :] * n + jnp.arange(n)[:, None]).reshape(-1)

    if each % (2 * SUBLANES):
        came = lax.all_to_all(raw_traces.reshape(n, each, length), "traces", 0, 0, tiled=True).reshape(rows, length)
        result = pl.pallas_call(
            functools.partial(block_kernel, taps, ()),
            grid=(rows // ROWS,),
            out_shape=jax.ShapeDtypeStruct((rows, length), jnp.float32),
            in_specs=[pl.BlockSpec((ROWS, length), lambda i: (i, 0))] + fixed,
            out_specs=pl.BlockSpec((ROWS, length), lambda i: (i, 0)),
            scratch_shapes=scratch(),
            compiler_params=params,
        )(came, jnp.take(bank, came_picks.reshape(-1), axis=0), fwd, inv, tw)
        return jnp.take(result, (channel_order % n) * each + channel_order // n, axis=0)

    hits = channel_order[None, :] == places[:, None]
    row_of = jnp.sum(jnp.where(hits, jnp.arange(rows)[None, :], 0), axis=1).reshape(n, 2, each // 2)
    group = ROWS // part if part < ROWS else 1
    split = raw_traces.reshape(n, 2, part, length)
    steps = n // group
    flops = pl.CostEstimate(flops=steps * ROWS * length * 1500, bytes_accessed=8 * steps * ROWS * length, transcendentals=0)

    came_raw = lax.all_to_all(first, "traces", 0, 0, tiled=True)
    own_rows = filter_index.reshape(n, 2, part)[:, 1].reshape(-1)
    done_here = pl.pallas_call(
        functools.partial(block_kernel, taps, (slice(None), 0)),
        grid=(steps,),
        out_shape=jax.ShapeDtypeStruct((n, part, length), jnp.float32),
        in_specs=[pl.BlockSpec((group, 1, part, length), lambda i: (i, 1, 0, 0))] + fixed,
        out_specs=pl.BlockSpec((group, part, length), lambda i: (i, 0, 0)),
        scratch_shapes=scratch(),
        compiler_params=params,
        cost_estimate=flops,
    )(split, jnp.take(bank, own_rows, axis=0), fwd, inv, tw)
    came_done = lax.all_to_all(done_here, "traces", 0, 0, tiled=True)
    came_rows = came_picks[:, :part].reshape(-1)
    filled = pl.pallas_call(
        functools.partial(place_kernel, taps),
        grid_spec=pltpu.PrefetchScalarGridSpec(
            num_scalar_prefetch=1,
            grid=(steps,),
            in_specs=[pl.BlockSpec((group, part, length), lambda i, *_: (i, 0, 0))] + fixed,
            out_specs=pl.BlockSpec(memory_space=pl.ANY),
            scratch_shapes=scratch()
            + [pltpu.VMEM((2, ROWS, length), jnp.float32), pltpu.SemaphoreType.DMA((2, ROWS))],
        ),
        out_shape=jax.ShapeDtypeStruct((rows, length), jnp.float32),
        compiler_params=params,
        cost_estimate=flops,
    )(row_of[:, 0].reshape(-1), came_raw, jnp.take(bank, came_rows, axis=0), fwd, inv, tw)
    return pl.pallas_call(
        settle_kernel,
        in_specs=[pl.BlockSpec(memory_space=pltpu.SMEM)] + [pl.BlockSpec(memory_space=pl.ANY)] * 2,
        out_specs=pl.BlockSpec(memory_space=pl.ANY),
        out_shape=jax.ShapeDtypeStruct((rows, length), jnp.float32),
        scratch_shapes=[
            pltpu.VMEM((n, part, length), jnp.float32),
            pltpu.SemaphoreType.DMA((n,)),
            pltpu.SemaphoreType.DMA((n, part)),
        ],
        input_output_aliases={2: 0},
        compiler_params=params,
    )(row_of[:, 1].reshape(-1), came_done, filled)


def solution(mesh):
    placed = (
        P(("groups", "traces"), None),
        P(("groups", "traces")),
        P("groups"),
        P("traces", None),
        P("traces"),
    )
    return jax.shard_map(
        local, mesh=mesh, in_specs=placed, out_specs=P(("groups", "traces"), None), check_vma=False
    )
```
